32 devices in a mesh: ctx: 4 (over x, core), head: 8 (over z, y).
Axes of the slice: x: 2, y: 2, z: 4, core: 2. Of those that a mesh axis runs over, the one named last changes fastest.
Arguments:
- layer_input: bfloat16 [1024, 8192], P('ctx'), may hold values from -6 to 6
- output_grad: bfloat16 [1024, 8192], P('ctx'), may hold values from -6 to 6
- routes: int32 [1024, 8], P('ctx'), may hold values from 0 to 31, all different within a row; in each aligned block of 256 rows (0 to 255, 256 to 511, ...) at most 128 rows name the same one
- route_gates: float32 [1024, 8], P('ctx'), may hold values from 0.05 to 0.3
- query_weight: bfloat16 [40, 8192, 128], P('head', 'ctx'), may hold values from -0.0625 to 0.0625
- output_weight: bfloat16 [40, 8192, 128], P('head', 'ctx'), may hold values from -0.0625 to 0.0625
- key_values: bfloat16 [8, 1024, 128], P('head', 'ctx'), may hold values from -96 to 96
Outputs:
- input_grad: bfloat16 [1024, 8192], P('ctx', 'head')
- keyvalue_grad: float32 [8, 1024, 128], P('head', 'ctx')
The draws below stay inside these ranges and needn't reach their ends.
Inputs may be any that keep to these rules, and one draw needn't show every extreme that they name: `routes`: each row names 8 different experts; in the 256 rows of one ctx block no expert is named more than 128 times, and some expert reaches 128.
All inputs are finite; a program needn't handle non-finite values.
Results may differ from the reference program's by a relative error of at most 0.015.
The reference program's roundings to bfloat16 on the way count: a program that leaves them out, or rounds other values in their place, can miss the bound.
Values may be sent and summed in bfloat16 or wider, within the bound.
A program may use at most 128 MiB of HBM per device.

```python
import math
import jax
import jax.numpy as jnp
import numpy as np
from jax import lax

D = 8192
HD = 128
TOP = 8
EXP_DEV = 4
TOK_DEV = 256
EXPERTS = 32
HEADS = 40
KVG = 4
CAP = 128
TOKENS = 1024
N_CTX = 4
N_HEAD = 8


def draw_key_values(key, part):
    normal_draw = jax.random.normal(key, (2 * KVG, TOKENS, HD), jnp.float32)
    normal_draw = jnp.clip(normal_draw, -4.0, 4.0)
    return normal_draw.astype(jnp.bfloat16)


def block_scale(own_key, extent, pieces, smallest, top_value):
    gain = 1.0
    for position, parts in pieces:
        draws = jax.random.uniform(jax.random.fold_in(jax.random.fold_in(own_key, 6), position), (parts,), jnp.float32, smallest / len(pieces), top_value / len(pieces))
        gain = gain * jnp.repeat(jnp.exp(draws), extent[position] // parts).reshape((-1,) + (1,) * (len(extent) - 1 - position))
    return gain


def assign_block(stream_key, own, number, rows, number_of, top, bound, skew):
    order = jax.random.permutation(stream_key, number_of)
    crowded, common = portions_of(number_of, rows * top, bound, skew, True), portions_of(number_of, rows * top, bound, skew, False)
    places = jnp.arange(number_of)

    def named(tallies, turn):
        used = int((tallies > 0).sum())
        fixed = max(1, used // 4)
        moved = fixed + (places - fixed + turn * (used - fixed)) % max(1, number_of - fixed)
        return jnp.zeros((number_of,), jnp.int32).at[order[jnp.where(places < fixed, places, moved)]].set(jnp.asarray(tallies, jnp.int32))

    tallies = jnp.where(number % 4 == 0, named(crowded, number // 4), named(common, number - number // 4 - 1))
    mixed = jax.random.permutation(jax.random.fold_in(own, 3), number_of)
    giver, receiver = mixed[0:number_of // 2 * 2:2], mixed[1:number_of // 2 * 2:2]
    margin = jnp.minimum(tallies[giver] - 1, bound - tallies[receiver]) // 2
    margin = jnp.where((giver == order[0]) | (receiver == order[0]) | (tallies[receiver] == 0), 0, jnp.maximum(margin, 0))
    moved = jax.random.randint(jax.random.fold_in(own, 4), (number_of // 2,), 0, 1 << 20) % (margin + 1)
    tallies = tallies.at[giver].add(-moved).at[receiver].add(moved)
    items = jnp.searchsorted(jnp.cumsum(tallies), jnp.arange(rows * top), side="right").astype(jnp.int32)
    listing = items.reshape(top, rows).T
    listing = listing[jax.random.permutation(jax.random.fold_in(own, 1), rows)]
    turn = jax.random.randint(jax.random.fold_in(own, 2), (rows, 1), 0, top)
    return jnp.take_along_axis(listing, (jnp.arange(top)[None, :] + turn) % top, axis=1)


def portions_of(number_of, total, most, lean, full):
    loads = [(1 << 20) // math.isqrt(standing ** lean) + 1 for standing in range(1, number_of + 1)]
    largest = most if full else min(most, max(-(-total // number_of), total * loads[0] // sum(loads)))
    least = 1 if total - largest >= number_of - 1 else 0
    counts, surplus = [largest] + [least] * (number_of - 1), total - largest - least * (number_of - 1)
    while surplus > 0:
        movable = [i for i in range(1, number_of) if counts[i] < largest] or [i for i in range(1, number_of) if counts[i] < most]
        whole, left = sum([loads[i] for i in movable]), surplus
        for i in movable:
            extra = min(most - counts[i], max(1, left * loads[i] // whole), surplus)
            counts[i] = counts[i] + extra
            surplus = surplus - extra
    return np.array(counts)


def scatter_about(rng, dims, deviation, limit, shards=(), kind=jnp.bfloat16):
    entries = deviation * jax.random.normal(rng, dims, jnp.float32)
    if shards:
        entries = entries * block_scale(rng, dims, shards, -0.22, 0.18)
    return jnp.clip(entries, -limit, limit).astype(kind)


def setup_inputs(seed: int = 0) -> dict:
    streams_of = jax.random.split(jax.random.key(seed), 8)
    layer_input = scatter_about(streams_of[0], (TOKENS, D), 1.0, 6.0, ((0, 4),))
    output_grad = scatter_about(streams_of[1], (TOKENS, D), 1.0, 6.0, ((0, 4),))
    routes_keys = jax.random.split(jax.random.fold_in(streams_of[2], 1), TOKENS // TOK_DEV)
    routes_turns = jax.random.permutation(jax.random.fold_in(streams_of[2], 3), TOKENS // TOK_DEV)
    routes = jax.vmap(lambda own, number: assign_block(jax.random.fold_in(streams_of[2], 2), own, number, TOK_DEV, EXPERTS, TOP, CAP, 2))(routes_keys, routes_turns).reshape((TOKENS, TOP))
    route_gates = jnp.clip(0.05 + 0.25 * jax.random.uniform(streams_of[3], (TOKENS, TOP), jnp.float32) ** block_scale(streams_of[3], (TOKENS, TOP), ((0, 4),), -0.2, 0.2), 0.05, 0.3)
    query_weight = scatter_about(streams_of[4], (HEADS, D, HD), D ** -0.5, 0.0625, ((0, 8), (1, 4)))
    output_weight = scatter_about(streams_of[5], (HEADS, D, HD), D ** -0.5, 0.0625, ((0, 8), (1, 4)))
    key_values = draw_key_values(jax.random.fold_in(streams_of[7], 71), 0)
    return dict(layer_input=layer_input, output_grad=output_grad, routes=routes, route_gates=route_gates, query_weight=query_weight, output_weight=output_weight, key_values=key_values)


PRECISE = lax.Precision.HIGHEST


def slot_table(route_rows, first_id, expert_count, slot_count):
    expert_ids = first_id + jnp.arange(expert_count, dtype=jnp.int32)
    matches = route_rows[:, :, None] == expert_ids[None, None, :]
    member = jnp.any(matches, axis=1).astype(jnp.int32)
    placed = jnp.cumsum(member, axis=0) - 1
    slot_map = (placed.T[:, None, :] == jnp.arange(slot_count, dtype=jnp.int32)[None, :, None]) & (member.T[:, None, :] == 1)
    return slot_map.astype(jnp.float32)


def expert_gate(route_rows, gate_rows, first_id, expert_count):
    expert_ids = first_id + jnp.arange(expert_count, dtype=jnp.int32)
    matches = route_rows[:, :, None] == expert_ids[None, None, :]
    return jnp.sum(jnp.where(matches, gate_rows[:, :, None], jnp.zeros_like(gate_rows)[:, :, None]), axis=1)


def attend(queries, query_place, key_rows, value_rows, key_place, head_grads):
    score_scale = queries.shape[1] ** -0.5
    scores = jnp.dot(queries, key_rows.T, preferred_element_type=jnp.float32) * score_scale
    scores = jnp.where(key_place[None, :] <= query_place[:, None], scores, -1e30)
    row_max = jnp.max(scores, axis=1, keepdims=True)
    raised = jnp.exp(scores - row_max)
    shares = raised / jnp.sum(raised, axis=1, keepdims=True)
    shares_low = shares.astype(jnp.bfloat16)
    outputs = jnp.dot(shares_low, value_rows, preferred_element_type=jnp.float32)
    share_grad = jnp.dot(head_grads, value_rows.T, preferred_element_type=jnp.float32)
    row_delta = jnp.sum(head_grads.astype(jnp.float32) * outputs, axis=1, keepdims=True)
    score_grad = (shares * (share_grad - row_delta) * score_scale).astype(jnp.bfloat16)
    query_grad = jnp.dot(score_grad, key_rows, preferred_element_type=jnp.float32).astype(jnp.bfloat16)
    key_grad = jnp.dot(score_grad.T, queries, preferred_element_type=jnp.float32)
    value_grad = jnp.dot(shares_low.T, head_grads, preferred_element_type=jnp.float32)
    return query_grad, key_grad, value_grad


def reference(layer_input, output_grad, routes, route_gates, query_weight, output_weight, key_values):
    per_block = EXP_DEV + 1
    key_place = jnp.arange(TOKENS, dtype=jnp.int32).astype(jnp.float32)
    place_blocks = key_place.reshape(N_CTX, TOK_DEV)
    input_blocks = layer_input.reshape(N_CTX, TOK_DEV, D).astype(jnp.float32)
    cotan_blocks = output_grad.reshape(N_CTX, TOK_DEV, D).astype(jnp.float32)
    route_blocks = routes.reshape(N_CTX, TOK_DEV, TOP)
    gate_blocks = route_gates.reshape(N_CTX, TOK_DEV, TOP)
    routed_rows = N_CTX * EXP_DEV * CAP

    def head_step(carry, head_index):
        input_acc, pair_acc = carry
        query_block = lax.dynamic_slice_in_dim(query_weight, head_index * per_block, per_block, 0).astype(jnp.float32)
        output_block = lax.dynamic_slice_in_dim(output_weight, head_index * per_block, per_block, 0).astype(jnp.float32)
        group_id = head_index // 2
        key_rows = lax.dynamic_index_in_dim(key_values, 2 * group_id, 0, keepdims=False)
        value_rows = lax.dynamic_index_in_dim(key_values, 2 * group_id + 1, 0, keepdims=False)
        first_id = head_index * EXP_DEV
        tables = jax.vmap(slot_table, in_axes=(0, None, None, None))(route_blocks, first_id, EXP_DEV, CAP)
        token_gates = jax.vmap(expert_gate, in_axes=(0, 0, None, None))(route_blocks, gate_blocks, first_id, EXP_DEV)
        picked_input = jnp.einsum('bjct,btd->bjcd', tables, input_blocks, precision=PRECISE).astype(jnp.bfloat16)
        routed_query = jnp.einsum('bjcd,jde->bjce', picked_input.astype(jnp.float32), query_block[:EXP_DEV], precision=PRECISE).astype(jnp.bfloat16)
        shared_query = jnp.einsum('btd,de->bte', input_blocks, query_block[EXP_DEV], precision=PRECISE).astype(jnp.bfloat16)
        picked_cotan = jnp.einsum('bjct,btd->bjcd', tables, cotan_blocks, precision=PRECISE).astype(jnp.bfloat16)
        slot_gate = jnp.einsum('bjct,btj->bjc', tables, token_gates, precision=PRECISE)
        routed_sum = jnp.einsum('bjcd,jde->bjce', picked_cotan.astype(jnp.float32), output_block[:EXP_DEV], precision=PRECISE)
        routed_cotan = (slot_gate[..., None] * routed_sum).astype(jnp.bfloat16)
        shared_cotan = jnp.einsum('btd,de->bte', cotan_blocks, output_block[EXP_DEV], precision=PRECISE).astype(jnp.bfloat16)
        routed_place = jnp.einsum('bjct,bt->bjc', tables, place_blocks, precision=PRECISE)
        queries = jnp.concatenate([routed_query.reshape(-1, HD), shared_query.reshape(-1, HD)], axis=0)
        query_place = jnp.concatenate([routed_place.reshape(-1), place_blocks.reshape(-1)], axis=0)
        head_grads = jnp.concatenate([routed_cotan.reshape(-1, HD), shared_cotan.reshape(-1, HD)], axis=0)
        query_grad, key_grad, value_grad = attend(queries, query_place, key_rows, value_rows, key_place, head_grads)
        routed_qgrad = query_grad[:routed_rows].reshape(N_CTX, EXP_DEV, CAP, HD).astype(jnp.float32)
        token_qgrad = jnp.einsum('bjct,bjce->btje', tables, routed_qgrad, precision=PRECISE).astype(jnp.bfloat16)
        shared_qgrad = query_grad[routed_rows:].reshape(N_CTX, TOK_DEV, 1, HD)
        every_qgrad = jnp.concatenate([token_qgrad, shared_qgrad], axis=2).reshape(TOKENS, per_block, HD)
        input_acc = input_acc + jnp.einsum('tje,jde->td', every_qgrad.astype(jnp.float32), query_block, precision=PRECISE)
        pair_acc = pair_acc.at[2 * group_id].add(key_grad).at[2 * group_id + 1].add(value_grad)
        return (input_acc, pair_acc), None

    initial = (jnp.zeros((TOKENS, D), jnp.float32), jnp.zeros((2 * KVG, TOKENS, HD), jnp.float32))
    (input_acc, pair_acc), ignored = lax.scan(head_step, initial, jnp.arange(N_HEAD, dtype=jnp.int32))
    return input_acc.astype(jnp.bfloat16), pair_acc
```

```python
import functools

import jax
import jax.numpy as jnp
from jax import lax
from jax.experimental import pallas as pl
from jax.experimental.pallas import tpu as pltpu
from jax.sharding import PartitionSpec as P

PRECISE = lax.Precision.HIGHEST


MESH = pl.DeviceIdType.MESH
ANY = pl.BlockSpec(memory_space=pl.ANY)


def partner(step, flip):
    ctx, ctx_count = lax.axis_index("ctx"), lax.axis_size("ctx")
    head = lax.axis_index("head")
    other = head + flip * (1 - 2 * (head % 2))
    return lax.rem(ctx + step, ctx_count), other


def paired_steps(ctx_count):
    return [(step, flip) for step in range(ctx_count) for flip in range(2) if step or flip]


def remote(source, target, send, recv, ctx, head):
    return pltpu.make_async_remote_copy(
        src_ref=source,
        dst_ref=target,
        send_sem=send,
        recv_sem=recv,
        device_id=(ctx, head),
        device_id_type=MESH,
    )


def greet(places):
    barrier = pltpu.get_barrier_semaphore()
    for place in places:
        pl.semaphore_signal(barrier, inc=1, device_id=place, device_id_type=MESH)
    pl.semaphore_wait(barrier, len(places))


def gather_kernel(
    pieces,
    query_ref,
    output_ref,
    pair_ref,
    query_out,
    output_out,
    pair_out,
    stage,
    load_sem,
    store_sem,
    side_send,
    side_recv,
    far_send,
    far_recv,
    hand_send,
    hand_recv,
    pair_send,
    pair_recv,
    pair_store,
):
    ctx_count = lax.axis_size("ctx")
    ctx, head = lax.axis_index("ctx"), lax.axis_index("head")
    chips = ctx_count // 2
    core = ctx % 2
    chip = ctx // 2
    sibling = ctx + 1 - 2 * core
    heads, depth, _ = query_ref.shape
    span = heads // pieces
    tokens = pair_ref.shape[1]
    sources, targets = (query_ref, output_ref), (query_out, output_out)
    chunks = [(which, piece) for which in range(2) for piece in range(pieces)]

    def staged(which, piece):
        return stage.at[which, pl.ds(piece * span, span)]

    def placed(which, piece, owner):
        return targets[which].at[
            pl.ds(piece * span, span), pl.ds(pl.multiple_of(owner * depth, depth), depth)
        ]

    loads = []
    for k, (which, piece) in enumerate(chunks):
        load = pltpu.make_async_copy(
            sources[which].at[pl.ds(piece * span, span)], staged(which, piece), load_sem.at[k]
        )
        load.start()
        loads.append(load)
    steps = paired_steps(ctx_count)
    greet([partner(step, flip) for step, flip in steps])

    far, ends = {}, []
    for k, (which, piece) in enumerate(chunks):
        loads[k].wait()
        for hop in range(1, chips):
            copy = remote(
                staged(which, piece),
                placed(which, piece, ctx),
                far_send.at[k, hop - 1],
                far_recv.at[k, hop - 1],
                lax.rem(chip + hop, chips) * 2 + core,
                head,
            )
            copy.start()
            far[k, hop] = copy
        side = remote(
            staged(which, piece),
            placed(which, piece, ctx),
            side_send.at[k],
            side_recv.at[k],
            sibling,
            head,
        )
        side.start()
        store = pltpu.make_async_copy(
            staged(which, piece), placed(which, piece, ctx), store_sem.at[k]
        )
        store.start()
        ends += [side, store]

    mine = pair_out.at[head % 2, pl.ds(pl.multiple_of(ctx * tokens, tokens), tokens)]
    for n, (step, flip) in enumerate(steps):
        copy = remote(
            pair_ref.at[0], mine, pair_send.at[n], pair_recv.at[n], *partner(step, flip)
        )
        copy.start()
        ends.append(copy)
    store = pltpu.make_async_copy(pair_ref.at[0], mine, pair_store)
    store.start()
    ends.append(store)

    for k, (which, piece) in enumerate(chunks):
        for hop in range(1, chips):
            far[k, hop].wait_recv()
            owner = lax.rem(chip - hop + chips, chips) * 2 + core
            block = placed(which, piece, owner)
            hand = remote(
                block, block, hand_send.at[k, hop - 1], hand_recv.at[k, hop - 1], sibling, head
            )
            hand.start()
            ends.append(hand)
    for copy in far.values():
        copy.wait_send()
    for copy in ends:
        copy.wait()


def gather_all(query_weight, output_weight, key_values):
    heads, depth, width = query_weight.shape
    ctx_count = lax.axis_size("ctx")
    chips = ctx_count // 2
    pieces = heads if chips <= 2 else 1
    full = jax.ShapeDtypeStruct((heads, depth * ctx_count, width), query_weight.dtype)
    pair = jax.ShapeDtypeStruct((2, key_values.shape[1] * ctx_count, width), key_values.dtype)
    count, hops, others = 2 * pieces, max(chips - 1, 1), 2 * ctx_count - 1
    dma = pltpu.SemaphoreType.DMA
    return pl.pallas_call(
        functools.partial(gather_kernel, pieces),
        out_shape=(full, full, pair),
        in_specs=[ANY, ANY, pl.BlockSpec(memory_space=pltpu.VMEM)],
        out_specs=(ANY, ANY, ANY),
        scratch_shapes=[pltpu.VMEM((2, heads, depth, width), query_weight.dtype)]
        + [dma((count,))] * 4
        + [dma((count, hops))] * 4
        + [dma((others,))] * 2
        + [dma],
        compiler_params=pltpu.CompilerParams(collective_id=0, has_side_effects=True),
    )(query_weight, output_weight, key_values)


def exchange_kernel(
    term_ref, grads_ref, term_out, grads_out, term_send, term_recv, grads_send, grads_recv
):
    ctx_count, head_count = lax.axis_size("ctx"), lax.axis_size("head")
    ctx, head = lax.axis_index("ctx"), lax.axis_index("head")
    columns = term_ref.shape[1] // head_count
    steps = paired_steps(ctx_count)
    others = [lax.rem(head + step, head_count) for step in range(1, head_count)]
    greet([(ctx, other) for other in others] + [partner(step, flip) for step, flip in steps])
    copies = []
    for n, other in enumerate(others):
        copies.append(
            remote(
                term_ref.at[:, pl.ds(pl.multiple_of(other * columns, columns), columns)],
                term_out.at[n],
                term_send.at[n],
                term_recv.at[n],
                ctx,
                other,
            )
        )
        copies[-1].start()
    for n, (step, flip) in enumerate(steps):
        to_ctx, to_head = partner(step, flip)
        copies.append(
            remote(
                grads_ref.at[to_head % 2, to_ctx],
                grads_out.at[n],
                grads_send.at[n],
                grads_recv.at[n],
                to_ctx,
                to_head,
            )
        )
        copies[-1].start()
    for copy in copies:
        copy.wait()


def exchange(term, grads):
    ctx_count, head_count = lax.axis_size("ctx"), lax.axis_size("head")
    others = 2 * ctx_count - 1
    dma = pltpu.SemaphoreType.DMA
    return pl.pallas_call(
        exchange_kernel,
        out_shape=(
            jax.ShapeDtypeStruct(
                (head_count - 1, term.shape[0], term.shape[1] // head_count), term.dtype
            ),
            jax.ShapeDtypeStruct((others,) + grads.shape[2:], grads.dtype),
        ),
        in_specs=[ANY, ANY],
        out_specs=(ANY, ANY),
        scratch_shapes=[dma((head_count - 1,))] * 2 + [dma((others,))] * 2,
        compiler_params=pltpu.CompilerParams(collective_id=1, has_side_effects=True),
    )(term, grads)


def slot_table(route_rows, first_id, expert_count, slot_count):
    expert_ids = first_id + jnp.arange(expert_count, dtype=jnp.int32)
    matches = route_rows[:, :, None] == expert_ids[None, None, :]
    member = jnp.any(matches, axis=1).astype(jnp.int32)
    placed = jnp.cumsum(member, axis=0) - 1
    slot_map = (placed.T[:, None, :] == jnp.arange(slot_count, dtype=jnp.int32)[None, :, None]) & (
        member.T[:, None, :] == 1
    )
    return slot_map.astype(jnp.float32)


def expert_gate(route_rows, gate_rows, first_id, expert_count):
    expert_ids = first_id + jnp.arange(expert_count, dtype=jnp.int32)
    matches = route_rows[:, :, None] == expert_ids[None, None, :]
    return jnp.sum(
        jnp.where(matches, gate_rows[:, :, None], jnp.zeros_like(gate_rows)[:, :, None]), axis=1
    )


def attend(queries, query_place, key_rows, value_rows, key_place, head_grads):
    score_scale = queries.shape[1] ** (-0.5)
    scores = jnp.dot(queries, key_rows.T, preferred_element_type=jnp.float32) * score_scale
    scores = jnp.where(key_place[None, :] <= query_place[:, None], scores, -1e30)
    row_max = jnp.max(scores, axis=1, keepdims=True)
    raised = jnp.exp(scores - row_max)
    shares = raised / jnp.sum(raised, axis=1, keepdims=True)
    shares_low = shares.astype(jnp.bfloat16)
    outputs = jnp.dot(shares_low, value_rows, preferred_element_type=jnp.float32)
    share_grad = jnp.dot(head_grads, value_rows.T, preferred_element_type=jnp.float32)
    row_delta = jnp.sum(head_grads.astype(jnp.float32) * outputs, axis=1, keepdims=True)
    score_grad = (shares * (share_grad - row_delta) * score_scale).astype(jnp.bfloat16)
    query_grad = jnp.dot(score_grad, key_rows, preferred_element_type=jnp.float32).astype(
        jnp.bfloat16
    )
    key_grad = jnp.dot(score_grad.T, queries, preferred_element_type=jnp.float32)
    value_grad = jnp.dot(shares_low.T, head_grads, preferred_element_type=jnp.float32)
    return (query_grad, key_grad, value_grad)


def per_device(
    layer_input, output_grad, routes, route_gates, query_weight, output_weight, key_values
):
    tokens_here = layer_input.shape[0]
    per_block = query_weight.shape[0]
    expert_count = per_block - 1
    head_width = query_weight.shape[2]
    ctx_count = lax.axis_size("ctx")
    head_count = lax.axis_size("head")
    slot_count = 2 * tokens_here * routes.shape[1] // (expert_count * head_count)
    ctx_index = lax.axis_index("ctx")
    head_index = lax.axis_index("head")
    token_place = (ctx_index * tokens_here + jnp.arange(tokens_here, dtype=jnp.int32)).astype(
        jnp.float32
    )
    key_place = jnp.arange(tokens_here * ctx_count, dtype=jnp.int32).astype(jnp.float32)
    first_id = head_index * expert_count
    tables = slot_table(routes, first_id, expert_count, slot_count)
    tables_low = tables.astype(jnp.bfloat16)
    token_gates = expert_gate(routes, route_gates, first_id, expert_count)
    query_full, output_full, pair_full = gather_all(query_weight, output_weight, key_values)
    key_rows, value_rows = pair_full[0], pair_full[1]
    picked_input = jnp.einsum(
        "jct,td->jcd", tables_low, layer_input, preferred_element_type=jnp.float32
    ).astype(jnp.bfloat16)
    routed_query = jnp.einsum(
        "jcd,jde->jce", picked_input, query_full[:expert_count], preferred_element_type=jnp.float32
    ).astype(jnp.bfloat16)
    shared_query = jnp.dot(
        layer_input, query_full[expert_count], preferred_element_type=jnp.float32
    ).astype(jnp.bfloat16)
    slot_gate = jnp.einsum("jct,tj->jc", tables, token_gates, precision=PRECISE)
    picked_cotan = jnp.einsum(
        "jct,td->jcd", tables_low, output_grad, preferred_element_type=jnp.float32
    ).astype(jnp.bfloat16)
    routed_sum = jnp.einsum(
        "jcd,jde->jce", picked_cotan, output_full[:expert_count], preferred_element_type=jnp.float32
    )
    shared_sum = jnp.dot(output_grad, output_full[expert_count], preferred_element_type=jnp.float32)
    routed_cotan = (slot_gate[:, :, None] * routed_sum).astype(jnp.bfloat16)
    shared_cotan = shared_sum.astype(jnp.bfloat16)
    routed_place = jnp.einsum("jct,t->jc", tables, token_place, precision=PRECISE)
    queries = jnp.concatenate([routed_query.reshape(-1, head_width), shared_query], axis=0)
    query_place = jnp.concatenate([routed_place.reshape(-1), token_place], axis=0)
    head_grads = jnp.concatenate([routed_cotan.reshape(-1, head_width), shared_cotan], axis=0)
    query_grad, key_grad, value_grad = attend(
        queries, query_place, key_rows, value_rows, key_place, head_grads
    )
    routed_rows = expert_count * slot_count
    routed_qgrad = query_grad[:routed_rows].reshape(expert_count, slot_count, head_width)
    token_qgrad = jnp.einsum(
        "jct,jce->tje", tables_low, routed_qgrad, preferred_element_type=jnp.float32
    ).astype(jnp.bfloat16)
    every_qgrad = jnp.concatenate(
        [token_qgrad, query_grad[routed_rows:].reshape(tokens_here, 1, head_width)], axis=1
    )
    input_term = jnp.einsum(
        "tje,jde->td", every_qgrad, query_full, preferred_element_type=jnp.float32
    )
    term = input_term.astype(jnp.bfloat16)
    grads = jnp.stack([key_grad, value_grad]).astype(jnp.bfloat16)
    grads = grads.reshape(2, ctx_count, tokens_here, head_width)
    term_got, grads_got = exchange(term, grads)
    columns = term.shape[1] // head_count
    own_term = lax.dynamic_slice_in_dim(term, head_index * columns, columns, 1)
    input_grad = (
        own_term.astype(jnp.float32) + jnp.sum(term_got.astype(jnp.float32), axis=0)
    ).astype(jnp.bfloat16)
    own_grads = grads[head_index % 2, ctx_index].astype(jnp.float32)
    kept_rows = own_grads + jnp.sum(grads_got.astype(jnp.float32), axis=0)
    return (input_grad, kept_rows[None])


def solution(mesh):
    in_specs = (
        P("ctx", None),
        P("ctx", None),
        P("ctx", None),
        P("ctx", None),
        P("head", "ctx", None),
        P("head", "ctx", None),
        P("head", "ctx", None),
    )
    out_specs = (P("ctx", "head"), P("head", "ctx", None))
    return jax.shard_map(
        per_device, mesh=mesh, in_specs=in_specs, out_specs=out_specs, check_vma=False
    )
```

```python
import functools

import jax
import jax.numpy as jnp
from jax import lax
from jax.experimental import pallas as pl
from jax.experimental.pallas import tpu as pltpu
from jax.sharding import PartitionSpec as P

PRECISE = lax.Precision.HIGHEST


MESH = pl.DeviceIdType.MESH
ANY = pl.BlockSpec(memory_space=pl.ANY)


def partner(step, flip):
    ctx, ctx_count = lax.axis_index("ctx"), lax.axis_size("ctx")
    head = lax.axis_index("head")
    other = head + flip * (1 - 2 * (head % 2))
    return lax.rem(ctx + step, ctx_count), other


def paired_steps(ctx_count):
    return [(step, flip) for step in range(ctx_count) for flip in range(2) if step or flip]


def remote(source, target, send, recv, ctx, head):
    return pltpu.make_async_remote_copy(
        src_ref=source,
        dst_ref=target,
        send_sem=send,
        recv_sem=recv,
        device_id=(ctx, head),
        device_id_type=MESH,
    )


def greet(places):
    barrier = pltpu.get_barrier_semaphore()
    for place in places:
        pl.semaphore_signal(barrier, inc=1, device_id=place, device_id_type=MESH)
    pl.semaphore_wait(barrier, len(places))


def gather_kernel(
    pieces,
    query_ref,
    output_ref,
    pair_ref,
    query_out,
    output_out,
    pair_out,
    stage,
    load_sem,
    store_sem,
    side_send,
    side_recv,
    far_send,
    far_recv,
    hand_send,
    hand_recv,
    pair_send,
    pair_recv,
    pair_store,
):
    ctx_count = lax.axis_size("ctx")
    ctx, head = lax.axis_index("ctx"), lax.axis_index("head")
    chips = ctx_count // 2
    core = ctx % 2
    chip = ctx // 2
    sibling = ctx + 1 - 2 * core
    heads, depth, _ = query_ref.shape
    span = heads // pieces
    tokens = pair_ref.shape[1]
    sources, targets = (query_ref, output_ref), (query_out, output_out)
    chunks = [(which, piece) for which in range(2) for piece in range(pieces)]

    def staged(which, piece):
        return stage.at[which, pl.ds(piece * span, span)]

    def placed(which, piece, owner):
        return targets[which].at[
            pl.ds(piece * span, span), pl.ds(pl.multiple_of(owner * depth, depth), depth)
        ]

    loads = []
    for k, (which, piece) in enumerate(chunks):
        load = pltpu.make_async_copy(
            sources[which].at[pl.ds(piece * span, span)], staged(which, piece), load_sem.at[k]
        )
        load.start()
        loads.append(load)
    steps = paired_steps(ctx_count)
    greet([partner(step, flip) for step, flip in steps])

    far, ends = {}, []
    for k, (which, piece) in enumerate(chunks):
        loads[k].wait()
        for hop in range(1, chips):
            copy = remote(
                staged(which, piece),
                placed(which, piece, ctx),
                far_send.at[k, hop - 1],
                far_recv.at[k, hop - 1],
                lax.rem(chip + hop, chips) * 2 + core,
                head,
            )
            copy.start()
            far[k, hop] = copy
        side = remote(
            staged(which, piece),
            placed(which, piece, ctx),
            side_send.at[k],
            side_recv.at[k],
            sibling,
            head,
        )
        side.start()
        store = pltpu.make_async_copy(
            staged(which, piece), placed(which, piece, ctx), store_sem.at[k]
        )
        store.start()
        ends += [side, store]

    mine = pair_out.at[head % 2, pl.ds(pl.multiple_of(ctx * tokens, tokens), tokens)]
    for n, (step, flip) in enumerate(steps):
        copy = remote(
            pair_ref.at[0], mine, pair_send.at[n], pair_recv.at[n], *partner(step, flip)
        )
        copy.start()
        ends.append(copy)
    store = pltpu.make_async_copy(pair_ref.at[0], mine, pair_store)
    store.start()
    ends.append(store)

    for k, (which, piece) in enumerate(chunks):
        for hop in range(1, chips):
            far[k, hop].wait_recv()
            owner = lax.rem(chip - hop + chips, chips) * 2 + core
            block = placed(which, piece, owner)
            hand = remote(
                block, block, hand_send.at[k, hop - 1], hand_recv.at[k, hop - 1], sibling, head
            )
            hand.start()
            ends.append(hand)
    for copy in far.values():
        copy.wait_send()
    for copy in ends:
        copy.wait()


def gather_all(query_weight, output_weight, key_values):
    heads, depth, width = query_weight.shape
    ctx_count = lax.axis_size("ctx")
    chips = ctx_count // 2
    pieces = heads if chips <= 2 else 1
    full = jax.ShapeDtypeStruct((heads, depth * ctx_count, width), query_weight.dtype)
    pair = jax.ShapeDtypeStruct((2, key_values.shape[1] * ctx_count, width), key_values.dtype)
    count, hops, others = 2 * pieces, max(chips - 1, 1), 2 * ctx_count - 1
    dma = pltpu.SemaphoreType.DMA
    return pl.pallas_call(
        functools.partial(gather_kernel, pieces),
        out_shape=(full, full, pair),
        in_specs=[ANY, ANY, pl.BlockSpec(memory_space=pltpu.VMEM)],
        out_specs=(ANY, ANY, ANY),
        scratch_shapes=[pltpu.VMEM((2, heads, depth, width), query_weight.dtype)]
        + [dma((count,))] * 4
        + [dma((count, hops))] * 4
        + [dma((others,))] * 2
        + [dma],
        compiler_params=pltpu.CompilerParams(collective_id=0, has_side_effects=True),
    )(query_weight, output_weight, key_values)


def exchange_kernel(
    term_ref, grads_ref, term_out, grads_out, relay_out, term_send, term_recv, grads_send, grads_recv
):
    ctx_count, head_count = lax.axis_size("ctx"), lax.axis_size("head")
    ctx, head = lax.axis_index("ctx"), lax.axis_index("head")
    columns = term_ref.shape[1] // head_count
    steps = paired_steps(ctx_count)
    others = [lax.rem(head + step, head_count) for step in range(1, head_count)]
    greet([(ctx, other) for other in others] + [partner(step, flip) for step, flip in steps])
    copies = []
    half, last = head_count // 2, head_count - 1
    relay = lax.rem(head + head_count - half // 2, head_count)
    opposite = pl.ds(pl.multiple_of(others[half - 1] * columns, columns), columns)
    first = remote(
        term_ref.at[:, opposite], relay_out, term_send.at[last], term_recv.at[last], ctx, relay
    )
    first.start()
    for n, other in enumerate(others):
        if n == half - 1:
            continue
        copies.append(
            remote(
                term_ref.at[:, pl.ds(pl.multiple_of(other * columns, columns), columns)],
                term_out.at[n],
                term_send.at[n],
                term_recv.at[n],
                ctx,
                other,
            )
        )
        copies[-1].start()
    for n, (step, flip) in enumerate(steps):
        to_ctx, to_head = partner(step, flip)
        copies.append(
            remote(
                grads_ref.at[to_head % 2, to_ctx],
                grads_out.at[n],
                grads_send.at[n],
                grads_recv.at[n],
                to_ctx,
                to_head,
            )
        )
        copies[-1].start()
    first.wait_recv()
    second = remote(
        relay_out,
        term_out.at[half - 1],
        term_send.at[half - 1],
        term_recv.at[half - 1],
        ctx,
        relay,
    )
    second.start()
    first.wait_send()
    copies.append(second)
    for copy in copies:
        copy.wait()


def exchange(term, grads):
    ctx_count, head_count = lax.axis_size("ctx"), lax.axis_size("head")
    others = 2 * ctx_count - 1
    dma = pltpu.SemaphoreType.DMA
    return pl.pallas_call(
        exchange_kernel,
        out_shape=(
            jax.ShapeDtypeStruct(
                (head_count - 1, term.shape[0], term.shape[1] // head_count), term.dtype
            ),
            jax.ShapeDtypeStruct((others,) + grads.shape[2:], grads.dtype),
            jax.ShapeDtypeStruct((term.shape[0], term.shape[1] // head_count), term.dtype),
        ),
        in_specs=[ANY, ANY],
        out_specs=(ANY, ANY, ANY),
        scratch_shapes=[dma((head_count,))] * 2 + [dma((others,))] * 2,
        compiler_params=pltpu.CompilerParams(collective_id=1, has_side_effects=True),
    )(term, grads)


def slot_table(route_rows, first_id, expert_count, slot_count):
    expert_ids = first_id + jnp.arange(expert_count, dtype=jnp.int32)
    matches = route_rows[:, :, None] == expert_ids[None, None, :]
    member = jnp.any(matches, axis=1).astype(jnp.int32)
    placed = jnp.cumsum(member, axis=0) - 1
    slot_map = (placed.T[:, None, :] == jnp.arange(slot_count, dtype=jnp.int32)[None, :, None]) & (
        member.T[:, None, :] == 1
    )
    return slot_map.astype(jnp.float32)


def expert_gate(route_rows, gate_rows, first_id, expert_count):
    expert_ids = first_id + jnp.arange(expert_count, dtype=jnp.int32)
    matches = route_rows[:, :, None] == expert_ids[None, None, :]
    return jnp.sum(
        jnp.where(matches, gate_rows[:, :, None], jnp.zeros_like(gate_rows)[:, :, None]), axis=1
    )


def attend(queries, query_place, key_rows, value_rows, key_place, head_grads):
    score_scale = queries.shape[1] ** (-0.5)
    scores = jnp.dot(queries, key_rows.T, preferred_element_type=jnp.float32) * score_scale
    scores = jnp.where(key_place[None, :] <= query_place[:, None], scores, -1e30)
    row_max = jnp.max(scores, axis=1, keepdims=True)
    raised = jnp.exp(scores - row_max)
    shares = raised / jnp.sum(raised, axis=1, keepdims=True)
    shares_low = shares.astype(jnp.bfloat16)
    outputs = jnp.dot(shares_low, value_rows, preferred_element_type=jnp.float32)
    share_grad = jnp.dot(head_grads, value_rows.T, preferred_element_type=jnp.float32)
    row_delta = jnp.sum(head_grads.astype(jnp.float32) * outputs, axis=1, keepdims=True)
    score_grad = (shares * (share_grad - row_delta) * score_scale).astype(jnp.bfloat16)
    query_grad = jnp.dot(score_grad, key_rows, preferred_element_type=jnp.float32).astype(
        jnp.bfloat16
    )
    key_grad = jnp.dot(score_grad.T, queries, preferred_element_type=jnp.float32)
    value_grad = jnp.dot(shares_low.T, head_grads, preferred_element_type=jnp.float32)
    return (query_grad, key_grad, value_grad)


def per_device(
    layer_input, output_grad, routes, route_gates, query_weight, output_weight, key_values
):
    tokens_here = layer_input.shape[0]
    per_block = query_weight.shape[0]
    expert_count = per_block - 1
    head_width = query_weight.shape[2]
    ctx_count = lax.axis_size("ctx")
    head_count = lax.axis_size("head")
    slot_count = 2 * tokens_here * routes.shape[1] // (expert_count * head_count)
    ctx_index = lax.axis_index("ctx")
    head_index = lax.axis_index("head")
    token_place = (ctx_index * tokens_here + jnp.arange(tokens_here, dtype=jnp.int32)).astype(
        jnp.float32
    )
    key_place = jnp.arange(tokens_here * ctx_count, dtype=jnp.int32).astype(jnp.float32)
    first_id = head_index * expert_count
    tables = slot_table(routes, first_id, expert_count, slot_count)
    tables_low = tables.astype(jnp.bfloat16)
    token_gates = expert_gate(routes, route_gates, first_id, expert_count)
    query_full, output_full, pair_full = gather_all(query_weight, output_weight, key_values)
    key_rows, value_rows = pair_full[0], pair_full[1]
    picked_input = jnp.einsum(
        "jct,td->jcd", tables_low, layer_input, preferred_element_type=jnp.float32
    ).astype(jnp.bfloat16)
    routed_query = jnp.einsum(
        "jcd,jde->jce", picked_input, query_full[:expert_count], preferred_element_type=jnp.float32
    ).astype(jnp.bfloat16)
    shared_query = jnp.dot(
        layer_input, query_full[expert_count], preferred_element_type=jnp.float32
    ).astype(jnp.bfloat16)
    slot_gate = jnp.einsum("jct,tj->jc", tables, token_gates, precision=PRECISE)
    picked_cotan = jnp.einsum(
        "jct,td->jcd", tables_low, output_grad, preferred_element_type=jnp.float32
    ).astype(jnp.bfloat16)
    routed_sum = jnp.einsum(
        "jcd,jde->jce", picked_cotan, output_full[:expert_count], preferred_element_type=jnp.float32
    )
    shared_sum = jnp.dot(output_grad, output_full[expert_count], preferred_element_type=jnp.float32)
    routed_cotan = (slot_gate[:, :, None] * routed_sum).astype(jnp.bfloat16)
    shared_cotan = shared_sum.astype(jnp.bfloat16)
    routed_place = jnp.einsum("jct,t->jc", tables, token_place, precision=PRECISE)
    queries = jnp.concatenate([routed_query.reshape(-1, head_width), shared_query], axis=0)
    query_place = jnp.concatenate([routed_place.reshape(-1), token_place], axis=0)
    head_grads = jnp.concatenate([routed_cotan.reshape(-1, head_width), shared_cotan], axis=0)
    query_grad, key_grad, value_grad = attend(
        queries, query_place, key_rows, value_rows, key_place, head_grads
    )
    routed_rows = expert_count * slot_count
    routed_qgrad = query_grad[:routed_rows].reshape(expert_count, slot_count, head_width)
    token_qgrad = jnp.einsum(
        "jct,jce->tje", tables_low, routed_qgrad, preferred_element_type=jnp.float32
    ).astype(jnp.bfloat16)
    every_qgrad = jnp.concatenate(
        [token_qgrad, query_grad[routed_rows:].reshape(tokens_here, 1, head_width)], axis=1
    )
    input_term = jnp.einsum(
        "tje,jde->td", every_qgrad, query_full, preferred_element_type=jnp.float32
    )
    term = input_term.astype(jnp.bfloat16)
    grads = jnp.stack([key_grad, value_grad]).astype(jnp.bfloat16)
    grads = grads.reshape(2, ctx_count, tokens_here, head_width)
    term_got, grads_got, _ = exchange(term, grads)
    columns = term.shape[1] // head_count
    own_term = lax.dynamic_slice_in_dim(term, head_index * columns, columns, 1)
    input_grad = (
        own_term.astype(jnp.float32) + jnp.sum(term_got.astype(jnp.float32), axis=0)
    ).astype(jnp.bfloat16)
    own_grads = grads[head_index % 2, ctx_index].astype(jnp.float32)
    kept_rows = own_grads + jnp.sum(grads_got.astype(jnp.float32), axis=0)
    return (input_grad, kept_rows[None])


def solution(mesh):
    in_specs = (
        P("ctx", None),
        P("ctx", None),
        P("ctx", None),
        P("ctx", None),
        P("head", "ctx", None),
        P("head", "ctx", None),
        P("head", "ctx", None),
    )
    out_specs = (P("ctx", "head"), P("head", "ctx", None))
    return jax.shard_map(
        per_device, mesh=mesh, in_specs=in_specs, out_specs=out_specs, check_vma=False
    )
```
